32 devices in a mesh: dp: 2 (over core), tvoc: 4 (over y, x), svoc: 4 (over z).
Axes of the slice: x: 2, y: 2, z: 4, core: 2. Of those that a mesh axis runs over, the one named last changes fastest.
Arguments:
- teacher_probs: bfloat16 [256, 20480], P('dp', 'tvoc'), may hold values from 0 to 1, as said below
- block_values: bfloat16 [4, 4, 24, 128, 128], P('tvoc', 'svoc'), may hold values from 0.0099487305 to 1
- block_index: int32 [4, 4, 24, 2], P('tvoc', 'svoc'), may hold values from 0 to 39, as said below
- block_count: int32 [4, 4], P('tvoc', 'svoc'), may hold values from 5 to 24, as said below
- hidden: bfloat16 [256, 3072], P('dp'), may hold values from -48 to 48
- student_weight: bfloat16 [3072, 8192], P(None, ('tvoc', 'svoc')), may hold values from -0.15 to 0.15
Outputs:
- divergence: float32 [256], P('dp')
- grad_weight: bfloat16 [3072, 8192], P('dp', ('tvoc', 'svoc'))
- grad_hidden: float32 [256, 3072], P('dp', ('tvoc', 'svoc'))
The draws below stay inside these ranges and needn't reach their ends.
Inputs may be any that keep to these rules, and one draw needn't show every extreme that they name: `teacher_probs`: each row sums to one and every entry is positive. `block_index`: entry [i, j, s, 0] is a teacher block of shard i, entry [i, j, s, 1] is c as in the reference program. The live slots of one device name at most 2 distinct c with the same c // 4, and some value of c // 4 reaches 2 on every device. Several live slots may name the same c, with the same or another teacher block. `block_count`: the live slots are the first ones; some device has all 24 live.
All inputs are finite; a program needn't handle non-finite values.
Results may differ from the reference program's by a relative error of at most 0.013.
Values may be sent and summed in bfloat16 or wider, within the bound.
A program may use at most 64 MiB of HBM per device.

```python
import math
import jax
import jax.numpy as jnp
from jax import lax

D = 3072
BLK = 128
TVB_DEV = 40
SVB_DEV = 4
SLOTS = 24
CAP = 2
TOKENS = 256
TEACHER_VOCAB = 20480
STUDENT_VOCAB = 8192
N_TVOC = 4
N_SVOC = 4


weight_limit = 0.1484375


def index_plan(key):
    base_key = jax.random.fold_in(key, 11)
    lowest = N_TVOC * (CAP - 1) + 1
    spread = SLOTS - lowest
    pair_total = N_TVOC * CAP

    def draw_device(device_key):
        pick_key, order_key, row_key, count_key, source_key, coin_key = jax.random.split(device_key, 6)
        pick_keys = jax.random.split(pick_key, N_TVOC)
        chosen = jax.vmap(lambda single_key: jax.random.permutation(single_key, SVB_DEV)[:CAP])(pick_keys)
        order = jax.random.permutation(order_key, pair_total)
        slot_range = jnp.arange(SLOTS, dtype=jnp.int32)
        fresh = order[slot_range % pair_total]
        source = jax.random.randint(source_key, (SLOTS,), 0, lowest)
        coin = jax.random.randint(coin_key, (SLOTS,), 0, 2) == 1
        pairing = jnp.where((slot_range >= lowest) & coin, order[source], fresh)
        owner = pairing // CAP
        within = pairing % CAP
        columns = owner * SVB_DEV + chosen[owner, within]
        teacher_rows = jax.random.randint(row_key, (SLOTS,), 0, TVB_DEV)
        offset = jax.random.randint(count_key, (), 0, spread + 1)
        count = SLOTS - offset * offset // max(spread, 1)
        return (jnp.stack([teacher_rows, columns], axis=-1).astype(jnp.int32), count.astype(jnp.int32))
    device_keys = jax.random.split(base_key, N_TVOC * N_SVOC)
    indices, counts = jax.vmap(draw_device)(device_keys)
    fullest = jax.random.randint(jax.random.fold_in(base_key, 5), (), 0, N_TVOC * N_SVOC)
    counts = jnp.where(jnp.arange(N_TVOC * N_SVOC) == fullest, SLOTS, counts)
    return (indices.reshape(N_TVOC, N_SVOC, SLOTS, 2), counts.reshape(N_TVOC, N_SVOC).astype(jnp.int32))


def draw_block_index(key, part):
    return index_plan(key)[0]


def draw_block_count(key, part):
    return index_plan(key)[1]


def weight_columns(key, chosen):
    column_key = jax.random.fold_in(key, 31)

    def single(column):
        return jax.random.normal(jax.random.fold_in(column_key, column), (D,), jnp.float32)
    return jax.vmap(single)(chosen) / math.sqrt(D)


def draw_student_weight(key, part):
    columns = weight_columns(key, jnp.arange(STUDENT_VOCAB, dtype=jnp.int32))
    return jnp.clip(columns.T, -weight_limit, weight_limit).astype(jnp.bfloat16)


def draw_hidden(key, part):
    base_key = jax.random.fold_in(key, 41)
    noise_key = jax.random.fold_in(base_key, 0)
    states = jax.random.normal(noise_key, (TOKENS, D), jnp.float32)
    return jnp.clip(states, -48.0, 48.0).astype(jnp.bfloat16)


def draw_teacher_probs(key, part):
    noise_key, column_key = jax.random.split(jax.random.fold_in(key, 21), 2)
    shape = (TOKENS, TEACHER_VOCAB)
    column_bias = jax.random.normal(column_key, (1, TEACHER_VOCAB), jnp.float32)
    scores = 1.5 * jax.random.normal(noise_key, shape, jnp.float32) + column_bias
    return jax.nn.softmax(scores, axis=-1).astype(jnp.bfloat16)


def levels(stream_key, shape, cuts, least, top_value):
    level = 1.0
    for position, parts in cuts:
        steps = jax.random.uniform(jax.random.fold_in(jax.random.fold_in(stream_key, 6), position), (parts,), jnp.float32, least / len(cuts), top_value / len(cuts))
        level = level * jnp.repeat(jnp.exp(steps), shape[position] // parts).reshape((-1,) + (1,) * (len(shape) - 1 - position))
    return level


def setup_inputs(seed: int = 0) -> dict:
    streams_of = jax.random.split(jax.random.key(seed), 7)
    return {
        "teacher_probs": draw_teacher_probs(jax.random.fold_in(streams_of[6], 71), 0),
        "block_values": jnp.clip(jnp.exp(math.log(1.0) - 4.61031033 * jax.random.uniform(streams_of[1], (N_TVOC, N_SVOC, SLOTS, BLK, BLK), jnp.float32) ** levels(streams_of[1], (N_TVOC, N_SVOC, SLOTS, BLK, BLK), ((0, 4), (1, 4)), -0.2, 0.2)), 0.0099487305, 1.0).astype(jnp.bfloat16),
        "block_index": draw_block_index(jax.random.fold_in(streams_of[6], 71), 0),
        "block_count": draw_block_count(jax.random.fold_in(streams_of[6], 71), 0),
        "hidden": draw_hidden(jax.random.fold_in(streams_of[6], 71), 0),
        "student_weight": draw_student_weight(jax.random.fold_in(streams_of[6], 71), 0),
    }


def reference(teacher_probs, block_values, block_index, block_count, hidden, student_weight):
    loss_scale = 128.0
    owned = N_TVOC * SVB_DEV
    shard_width = SVB_DEV * BLK

    def device_partial(teacher_shard, student_shard):
        shard_probs = lax.dynamic_slice_in_dim(teacher_probs, teacher_shard * (TVB_DEV * BLK), TVB_DEV * BLK, 1)
        shard_probs = shard_probs.reshape(TOKENS, TVB_DEV, BLK)
        indices = block_index[teacher_shard, student_shard]
        entries = block_values[teacher_shard, student_shard]
        occupied = (jnp.arange(SLOTS, dtype=jnp.int32) < block_count[teacher_shard, student_shard]).astype(jnp.float32)
        picked = jnp.take(shard_probs, indices[:, 0], axis=1)
        mapped = jnp.einsum('tsk,skc->stc', picked.astype(jnp.float32), entries.astype(jnp.float32))
        mapped = mapped * occupied[:, None, None]
        summed = jnp.zeros((owned, TOKENS, BLK), jnp.float32).at[indices[:, 1]].add(mapped)
        rounded = lax.optimization_barrier(summed.astype(jnp.bfloat16))
        return jnp.transpose(rounded.astype(jnp.float32), (1, 0, 2))

    def per_student(student_shard):

        def accumulate(running, teacher_shard):
            return (running + device_partial(teacher_shard, student_shard), None)
        running, _ = lax.scan(accumulate, jnp.zeros((TOKENS, owned, BLK), jnp.float32), jnp.arange(N_TVOC, dtype=jnp.int32))
        return running
    stacked = lax.map(per_student, jnp.arange(N_SVOC, dtype=jnp.int32))
    stacked = stacked.reshape(N_SVOC, TOKENS, N_TVOC, shard_width)
    teacher_mass = jnp.transpose(stacked, (1, 2, 0, 3)).reshape(TOKENS, STUDENT_VOCAB)
    logits = jnp.dot(hidden.astype(jnp.float32), student_weight.astype(jnp.float32), preferred_element_type=jnp.float32)
    largest = jnp.max(logits, axis=1)
    shifted = jnp.exp(logits - largest[:, None])
    total = jnp.sum(shifted, axis=1)
    mass_sum = jnp.sum(teacher_mass, axis=1)
    target = teacher_mass / mass_sum[:, None]
    positive = target > 0
    log_target = jnp.log(jnp.where(positive, target, 1.0))
    terms = jnp.where(positive, target * log_target, 0.0) - target * (logits - largest[:, None] - jnp.log(total)[:, None])
    divergence = jnp.sum(terms, axis=1)
    logit_grad = (loss_scale * (shifted / total[:, None] - target)).astype(jnp.bfloat16)
    grad_weight = jnp.dot(hidden.T.astype(jnp.float32), logit_grad.astype(jnp.float32), preferred_element_type=jnp.float32).astype(jnp.bfloat16)
    grad_hidden = jnp.dot(logit_grad.astype(jnp.float32), student_weight.T.astype(jnp.float32), preferred_element_type=jnp.float32)
    return (divergence, grad_weight, grad_hidden)
```

```python
import functools

import jax
import jax.numpy as jnp
from jax import lax
from jax.experimental import pallas as pl
from jax.experimental.pallas import tpu as pltpu
from jax.sharding import PartitionSpec as P

loss_scale = 128.0
cap = 2
tag_rows = 16
MESH = pl.DeviceIdType.MESH
f32, bf16 = jnp.float32, jnp.bfloat16


def packer(
    n_t, per_owner, idx_s, cnt_s, idx_v, teacher_hbm, values_hbm,
    packed, teacher, values, mapped, targets, tags, load_sem,
):
    tokens = teacher.shape[0]
    slots, blk = values.shape[0], values.shape[1]
    loads = (
        pltpu.make_async_copy(teacher_hbm, teacher, load_sem.at[0]),
        pltpu.make_async_copy(values_hbm.at[0, 0], values, load_sem.at[1]),
    )
    for load in loads:
        load.start()

    lanes = targets.shape[1]
    lane = lax.broadcasted_iota(jnp.int32, (slots, lanes), 1)
    slot = lax.broadcasted_iota(jnp.int32, (slots, lanes), 0)
    hot = (idx_v[0, 0][:, 1:2] == lane) & (slot < cnt_s[0, 0])
    present = jnp.max(jnp.where(hot, 1.0, 0.0), axis=0, keepdims=True)
    r_iota = lax.broadcasted_iota(jnp.int32, (lanes, lanes), 0).astype(f32)
    c_iota = lax.broadcasted_iota(jnp.int32, (lanes, lanes), 1).astype(f32)
    r_own = jnp.floor((r_iota + 0.5) / per_owner)
    c_own = jnp.floor((c_iota + 0.5) / per_owner)
    below = jnp.where((r_own == c_own) & (r_iota < c_iota), 1.0, 0.0)
    rank = jnp.dot(jnp.broadcast_to(present, (8, lanes)), below, preferred_element_type=f32)[0:1]
    place = cap * c_own[0:1] + rank
    goal = jnp.sum(jnp.where(hot, place + 1.0, 0.0), axis=1, keepdims=True) - 1.0
    targets[...] = jnp.broadcast_to(goal, (slots, lanes))
    n_tags = tags.shape[0]
    t_iota = lax.broadcasted_iota(jnp.int32, (n_tags, lanes), 0).astype(f32)
    within = c_iota[0:1] - per_owner * c_own[0:1]
    tag = jnp.sum(jnp.where((present > 0.0) & (place == t_iota), within + 1.0, 0.0), axis=1, keepdims=True) - 1.0
    tags[...] = jnp.broadcast_to(tag, (n_tags, lanes))

    for load in loads:
        load.wait()
    for s in range(slots):
        row = idx_s[0, 0, s, 0]
        picked = teacher[:, pl.ds(pl.multiple_of(row * blk, blk), blk)]
        mapped[s] = jnp.dot(picked, values[s], preferred_element_type=f32)

    def pack(o):
        for k in range(cap):
            t = (o * cap + k).astype(f32)
            acc = jnp.zeros((tokens, blk), f32)
            for s in range(slots):
                acc = acc + jnp.where(targets[s:s + 1, 0:blk] == t, mapped[s], 0.0)
            packed[o, 0:tokens, k * blk:(k + 1) * blk] = acc.astype(bf16)
            packed[o, tokens:tokens + tag_rows, k * blk:(k + 1) * blk] = jnp.broadcast_to(
                tags[pl.ds(o * cap + k, 1), 0:blk], (tag_rows, blk)).astype(bf16)

    def step(o, carry):
        pack(o)
        return carry

    lax.fori_loop(0, n_t, step, 0)


def kernel(
    n_t, n_s, blk,
    packed, hidden_hbm, weight_hbm,
    div_ref, gw_ref, gh_ref,
    hidden, weight, peer_hidden, hid_t, landed, mass, logits, stats, grads, grad_t, gh_t, out1, in1, out2, in2,
    load_sem, ph_sem, pk_send, pk_recv, st_send, st_recv, lg_sem, s1, r1, s2, r2,
):
    d, i, j = lax.axis_index("dp"), lax.axis_index("tvoc"), lax.axis_index("svoc")
    n_d = 2
    n = n_t * n_s
    me = i * n_s + j
    other = n_d - 1 - d
    tokens, width = hidden.shape
    shard = weight.shape[1]
    per_owner = shard // blk
    half = width // n_d
    rows = width // n

    loads = [
        pltpu.make_async_copy(src, dst, load_sem.at[k])
        for k, (src, dst) in enumerate(
            ((hidden_hbm, hidden), (weight_hbm, weight))
        )
    ]
    for load in loads:
        load.start()

    def peer(q):
        r = lax.rem(me + q, n)
        return r, {"tvoc": r // n_s, "svoc": lax.rem(r, n_s)}

    barrier = pltpu.get_barrier_semaphore()

    def greet(q, carry):
        pl.semaphore_signal(barrier, inc=1, device_id=peer(q)[1], device_id_type=MESH)
        return carry

    lax.fori_loop(1, n, greet, 0)
    pl.semaphore_signal(barrier, inc=1, device_id={"dp": other}, device_id_type=MESH)

    for load in loads:
        load.wait()
    depth = 4 * blk
    logits[...] = jnp.zeros_like(logits)

    def logit_step(k, carry):
        at = pl.multiple_of(k * depth, depth)
        logits[...] += jnp.dot(hidden[:, pl.ds(at, depth)], weight[pl.ds(at, depth), :], preferred_element_type=f32)
        return carry

    lax.fori_loop(0, width // depth, logit_step, 0)

    pl.semaphore_wait(barrier, n)

    def hidden_copy():
        start = pl.multiple_of(other * half, blk)
        return pltpu.make_async_remote_copy(
            src_ref=hidden.at[:, pl.ds(start, half)], dst_ref=peer_hidden,
            send_sem=ph_sem.at[0], recv_sem=ph_sem.at[1],
            device_id={"dp": other}, device_id_type=MESH)

    def packed_copy(o, src):
        return pltpu.make_async_remote_copy(
            src_ref=packed.at[o], dst_ref=landed.at[src],
            send_sem=pk_send.at[o], recv_sem=pk_recv.at[src],
            device_id={"tvoc": o}, device_id_type=MESH)

    def pack_send(q, carry):
        o = lax.rem(i + q, n_t)
        packed_copy(o, i).start()
        return carry

    lax.fori_loop(1, n_t, pack_send, 0)
    hidden_copy().start()

    own_at = d * half

    def turn_own(k, carry):
        at = pl.multiple_of(k * blk, blk)
        tile = hidden[:, pl.ds(pl.multiple_of(own_at + at, blk), blk)].astype(f32)
        hid_t[pl.ds(at, blk), 0:tokens] = tile.T.astype(bf16)
        return carry

    lax.fori_loop(0, half // blk, turn_own, 0)

    def add_mass(ref, o, first):
        for b in range(per_owner):
            acc = jnp.zeros((tokens, blk), f32) if first else mass[:, b * blk:(b + 1) * blk]
            for k in range(cap):
                which = ref[o, tokens:tokens + 1, k * blk:(k + 1) * blk].astype(f32)
                part = ref[o, 0:tokens, k * blk:(k + 1) * blk].astype(f32)
                acc = acc + jnp.where(which == float(b), part, 0.0)
            mass[:, b * blk:(b + 1) * blk] = acc

    add_mass(packed, i, True)

    def take_mass(q, carry):
        o = lax.rem(i + q, n_t)
        packed_copy(o, o).wait_recv()
        add_mass(landed, o, False)
        return carry

    lax.fori_loop(1, n_t, take_mass, 0)

    lg = logits[...]
    tm = mass[...]
    top = jnp.max(lg, axis=1, keepdims=True)
    e = jnp.exp(lg - top)
    positive = tm > 0
    parts = (
        top,
        jnp.sum(e, axis=1, keepdims=True),
        jnp.sum(tm, axis=1, keepdims=True),
        jnp.sum(jnp.where(positive, tm * jnp.log(jnp.where(positive, tm, 1.0)), 0.0), axis=1, keepdims=True),
        jnp.sum(tm * lg, axis=1, keepdims=True),
    )
    spot = lax.broadcasted_iota(jnp.int32, (tokens, 128), 1)
    wide = jnp.zeros((tokens, 128), f32)
    for k, part in enumerate(parts):
        wide = jnp.where(spot == k, part, wide)
    stats[me] = wide.T[0:8]
    logits[...] = e

    def stat_copy(q, src):
        r, where = peer(q)
        return pltpu.make_async_remote_copy(
            src_ref=stats.at[me], dst_ref=stats.at[src],
            send_sem=st_send.at[q], recv_sem=st_recv.at[src],
            device_id=where, device_id_type=MESH)

    def stat_send(q, carry):
        stat_copy(q, me).start()
        return carry

    lax.fori_loop(1, n, stat_send, 0)

    hidden_copy().wait_recv()

    def turn_peer(k, carry):
        at = pl.multiple_of(k * blk, blk)
        hid_t[pl.ds(at, blk), tokens:2 * tokens] = peer_hidden[:, pl.ds(at, blk)].astype(f32).T.astype(bf16)
        return carry

    lax.fori_loop(0, half // blk, turn_peer, 0)

    def stat_wait(q, carry):
        stat_copy(q, peer(q)[0]).wait_recv()
        return carry

    lax.fori_loop(1, n, stat_wait, 0)
    st = stats[...]
    largest = jnp.max(st, axis=0)[0:1]
    scale = jnp.exp(st[:, 0:1, :] - largest[None])
    line = lax.broadcasted_iota(jnp.int32, st.shape, 1)
    sums = jnp.sum(jnp.where(line == 1, st * scale, st), axis=0)
    total, mass_sum, entropy, cross = sums[1:2], sums[2:3], sums[3:4], sums[4:5]
    div_ref[...] = entropy / mass_sum - jnp.log(mass_sum) - cross / mass_sum + largest + jnp.log(total)
    rows8 = lax.broadcasted_iota(jnp.int32, (128, tokens), 0)
    back = jnp.where(rows8 == 0, largest, jnp.where(rows8 == 1, loss_scale / total, loss_scale / mass_sum)).T
    factor = jnp.exp(top - back[:, 0:1]) * back[:, 1:2]
    g = logits[...] * factor - mass[...] * back[:, 2:3]
    grads[0:tokens, :] = g.astype(bf16)
    lg_copy = pltpu.make_async_remote_copy(
        src_ref=grads.at[pl.ds(0, tokens)], dst_ref=grads.at[pl.ds(tokens, tokens)],
        send_sem=lg_sem.at[0], recv_sem=lg_sem.at[1],
        device_id={"dp": other}, device_id_type=MESH)
    lg_copy.start()
    grad_t[...] = g.T.astype(bf16)

    tile = 2 * blk

    def gh_step(k, carry):
        at = pl.multiple_of(k * tile, tile)
        gh_t[pl.ds(at, tile), :] = jnp.dot(weight[pl.ds(at, tile), :], grad_t[...], preferred_element_type=f32)
        return carry

    lax.fori_loop(0, width // tile, gh_step, 0)

    def chunk(ii, jj):
        return gh_t[pl.ds(pl.multiple_of((ii * n_s + jj) * rows, 8), rows), :]

    def copy1(ii, jj, src):
        return pltpu.make_async_remote_copy(
            src_ref=out1.at[ii, jj], dst_ref=in1.at[src, jj],
            send_sem=s1.at[ii, jj], recv_sem=r1.at[src, jj],
            device_id={"tvoc": ii}, device_id_type=MESH)

    def copy2(jj, src):
        return pltpu.make_async_remote_copy(
            src_ref=out2.at[jj], dst_ref=in2.at[src],
            send_sem=s2.at[jj], recv_sem=r2.at[src],
            device_id={"svoc": jj}, device_id_type=MESH)

    def send1(p, carry):
        jj = lax.rem(j + p, n_s)

        def inner(q, c):
            ii = lax.rem(i + q, n_t)
            out1[ii, jj] = chunk(ii, jj).astype(bf16)
            copy1(ii, jj, i).start()
            return c

        return lax.fori_loop(1, n_t, inner, carry)

    lax.fori_loop(1, n_s + 1, send1, 0)

    lg_copy.wait_recv()

    def gw_step(k, carry):
        at = pl.multiple_of(k * blk, blk)
        gw_ref[pl.ds(at, blk), :] = jnp.dot(
            hid_t[pl.ds(at, blk), :], grads[...], preferred_element_type=f32).astype(bf16)
        return carry

    lax.fori_loop(0, half // blk, gw_step, 0)

    def gather1(jj):
        acc = chunk(i, jj)
        for q in range(1, n_t):
            ii = lax.rem(i + q, n_t)
            copy1(ii, jj, ii).wait_recv()
            acc = acc + in1[ii, jj].astype(f32)
        return acc

    def send2(p, carry):
        jj = lax.rem(j + p, n_s)
        out2[jj] = gather1(jj).astype(bf16)
        copy2(jj, j).start()
        return carry

    lax.fori_loop(1, n_s, send2, 0)
    acc = gather1(j)
    for p in range(1, n_s):
        jj = lax.rem(j + p, n_s)
        copy2(jj, jj).wait_recv()
        acc = acc + in2[jj].astype(f32)
    gh_ref[...] = acc

    hidden_copy().wait_send()
    lg_copy.wait_send()

    def drain_packed(q, carry):
        o = lax.rem(i + q, n_t)
        packed_copy(o, i).wait_send()
        return carry

    lax.fori_loop(1, n_t, drain_packed, 0)

    def drain_stats(q, carry):
        stat_copy(q, me).wait_send()
        return carry

    lax.fori_loop(1, n, drain_stats, 0)

    def drain1(p, carry):
        jj = lax.rem(j + p, n_s)

        def inner(q, c):
            copy1(lax.rem(i + q, n_t), jj, i).wait_send()
            return c

        return lax.fori_loop(1, n_t, inner, carry)

    lax.fori_loop(1, n_s + 1, drain1, 0)

    def drain2(p, carry):
        copy2(lax.rem(j + p, n_s), j).wait_send()
        return carry

    lax.fori_loop(1, n_s, drain2, 0)


def local(n_t, n_s, teacher_probs, block_values, block_index, block_count, hidden, student_weight):
    tokens, width = hidden.shape
    slots, blk = block_values.shape[2], block_values.shape[3]
    shard = student_weight.shape[1]
    half, rows, n = width // 2, width // (n_t * n_s), n_t * n_s
    lanes = -(-(n_t * (shard // blk)) // 128) * 128
    vmem, smem = pl.BlockSpec(memory_space=pltpu.VMEM), pl.BlockSpec(memory_space=pltpu.SMEM)
    hbm = pl.BlockSpec(memory_space=pltpu.HBM)
    DMA = pltpu.SemaphoreType.DMA
    parcel = (n_t, tokens + tag_rows, cap * blk)
    packed = pl.pallas_call(
        functools.partial(packer, n_t, shard // blk),
        out_shape=jax.ShapeDtypeStruct(parcel, bf16),
        in_specs=[smem, smem, vmem, hbm, hbm],
        out_specs=vmem,
        scratch_shapes=[
            pltpu.VMEM(teacher_probs.shape, bf16),
            pltpu.VMEM(block_values.shape[2:], bf16),
            pltpu.VMEM((slots, tokens, blk), f32),
            pltpu.VMEM((slots, lanes), f32),
            pltpu.VMEM((n_t * cap, lanes), f32),
            DMA((2,)),
        ],
        compiler_params=pltpu.CompilerParams(vmem_limit_bytes=32 * 1024 * 1024),
    )(block_index, block_count, block_index, teacher_probs, block_values)
    div, gw, gh = pl.pallas_call(
        functools.partial(kernel, n_t, n_s, blk),
        out_shape=(
            jax.ShapeDtypeStruct((1, tokens), f32),
            jax.ShapeDtypeStruct((half, shard), bf16),
            jax.ShapeDtypeStruct((rows, tokens), f32),
        ),
        in_specs=[vmem, hbm, hbm],
        out_specs=(vmem, vmem, vmem),
        scratch_shapes=[
            pltpu.VMEM(hidden.shape, bf16),
            pltpu.VMEM(student_weight.shape, bf16),
            pltpu.VMEM((tokens, half), bf16),
            pltpu.VMEM((half, 2 * tokens), bf16),
            pltpu.VMEM(parcel, bf16),
            pltpu.VMEM((tokens, shard), f32),
            pltpu.VMEM((tokens, shard), f32),
            pltpu.VMEM((n, 8, tokens), f32),
            pltpu.VMEM((2 * tokens, shard), bf16),
            pltpu.VMEM((shard, tokens), bf16),
            pltpu.VMEM((width, tokens), f32),
            pltpu.VMEM((n_t, n_s, rows, tokens), bf16),
            pltpu.VMEM((n_t, n_s, rows, tokens), bf16),
            pltpu.VMEM((n_s, rows, tokens), bf16),
            pltpu.VMEM((n_s, rows, tokens), bf16),
            DMA((2,)), DMA((2,)), DMA((n_t,)), DMA((n_t,)), DMA((n,)), DMA((n,)), DMA((2,)),
            DMA((n_t, n_s)), DMA((n_t, n_s)), DMA((n_s,)), DMA((n_s,)),
        ],
        compiler_params=pltpu.CompilerParams(
            collective_id=0, has_side_effects=True, vmem_limit_bytes=32 * 1024 * 1024),
    )(packed, hidden, student_weight)
    return div.reshape(tokens), gw, gh.T


def solution(mesh):
    return jax.shard_map(
        functools.partial(local, mesh.shape["tvoc"], mesh.shape["svoc"]),
        mesh=mesh,
        in_specs=(
            P("dp", "tvoc"),
            P("tvoc", "svoc", None, None, None),
            P("tvoc", "svoc", None, None),
            P("tvoc", "svoc"),
            P("dp", None),
            P(None, ("tvoc", "svoc")),
        ),
        out_specs=(P("dp"), P("dp", ("tvoc", "svoc")), P("dp", ("tvoc", "svoc"))),
        check_vma=False,
    )
```

```python
import functools

import jax
import jax.numpy as jnp
from jax import lax
from jax.experimental import pallas as pl
from jax.experimental.pallas import tpu as pltpu
from jax.sharding import PartitionSpec as P

loss_scale = 128.0
cap = 2
tag_rows = 16
MESH = pl.DeviceIdType.MESH
f32, bf16 = jnp.float32, jnp.bfloat16


def kernel(
    n_t, n_s, blk,
    idx_s, cnt_s, teacher_hbm, values_hbm, hidden_hbm, weight_hbm,
    div_ref, gw_ref, gh_ref,
    teacher, values, hidden, weight, peer_hidden, hid_t, mapped, targets, tags,
    packed, landed, mass, logits, shifted, stats, grads, grad_t, gh_t, own_t, out1, in1, out2, in2,
    block_sem, load_sem, ph_sem, pk_send, pk_recv, st_send, st_recv, lg_sem, s1, r1, s2, r2,
):
    d, i, j = lax.axis_index("dp"), lax.axis_index("tvoc"), lax.axis_index("svoc")
    n_d = 2
    n = n_t * n_s
    me = i * n_s + j
    other = n_d - 1 - d
    tokens, width = hidden.shape
    shard = weight.shape[1]
    per_owner = shard // blk
    half = width // n_d
    rows = width // n

    slots, blocks = values.shape[0], teacher.shape[0]
    loads = [
        pltpu.make_async_copy(src, dst, load_sem.at[k])
        for k, (src, dst) in enumerate(((values_hbm.at[0, 0], values), (hidden_hbm, hidden), (weight_hbm, weight)))
    ]
    loads[0].start()

    def block_load(b):
        return pltpu.make_async_copy(
            teacher_hbm.at[:, pl.ds(pl.multiple_of(b * blk, blk), blk)], teacher.at[b], block_sem.at[b])

    def block_start(b, carry):
        block_load(b).start()
        return carry

    lax.fori_loop(0, blocks, block_start, 0)
    loads[1].start()
    loads[2].start()

    def peer(q):
        r = lax.rem(me + q, n)
        return r, {"tvoc": r // n_s, "svoc": lax.rem(r, n_s)}

    barrier = pltpu.get_barrier_semaphore()

    def greet(q, carry):
        pl.semaphore_signal(barrier, inc=1, device_id=peer(q)[1], device_id_type=MESH)
        return carry

    lax.fori_loop(1, n, greet, 0)
    pl.semaphore_signal(barrier, inc=1, device_id={"dp": other}, device_id_type=MESH)

    lanes = targets.shape[1]
    lane = lax.broadcasted_iota(jnp.int32, (slots, lanes), 1)
    slot = lax.broadcasted_iota(jnp.int32, (slots, lanes), 0)
    column = jnp.zeros((slots, lanes), jnp.int32)
    for s in range(slots):
        column = jnp.where(slot == s, idx_s[0, 0, 1, s], column)
    hot = (column == lane) & (slot < cnt_s[0, 0])
    present = jnp.max(jnp.where(hot, 1.0, 0.0), axis=0, keepdims=True)
    r_iota = lax.broadcasted_iota(jnp.int32, (lanes, lanes), 0).astype(f32)
    c_iota = lax.broadcasted_iota(jnp.int32, (lanes, lanes), 1).astype(f32)
    r_own = jnp.floor((r_iota + 0.5) / per_owner)
    c_own = jnp.floor((c_iota + 0.5) / per_owner)
    below = jnp.where((r_own == c_own) & (r_iota < c_iota), 1.0, 0.0)
    rank = jnp.dot(jnp.broadcast_to(present, (8, lanes)), below, preferred_element_type=f32)[0:1]
    place = cap * c_own[0:1] + rank
    goal = jnp.sum(jnp.where(hot, place + 1.0, 0.0), axis=1, keepdims=True) - 1.0
    targets[...] = jnp.broadcast_to(goal, (slots, lanes))
    n_tags = tags.shape[0]
    t_iota = lax.broadcasted_iota(jnp.int32, (n_tags, lanes), 0).astype(f32)
    within = c_iota[0:1] - per_owner * c_own[0:1]
    tag = jnp.sum(jnp.where((present > 0.0) & (place == t_iota), within + 1.0, 0.0), axis=1, keepdims=True) - 1.0
    tags[...] = jnp.broadcast_to(tag, (n_tags, lanes))

    def block_wait(b, carry):
        block_load(b).wait()
        return carry

    loads[0].wait()
    lax.fori_loop(0, blocks, block_wait, 0)
    for s in range(slots):
        mapped[s] = jnp.dot(teacher[idx_s[0, 0, 0, s]], values[s], preferred_element_type=f32)

    def pack(q, carry):
        o = lax.rem(i + q, n_t)
        for k in range(cap):
            t = (o * cap + k).astype(f32)
            acc = jnp.zeros((tokens, blk), f32)
            for s in range(slots):
                acc = acc + jnp.where(targets[s:s + 1, 0:blk] == t, mapped[s], 0.0)
            packed[o, 0:tokens, k * blk:(k + 1) * blk] = acc.astype(bf16)
            packed[o, tokens:tokens + tag_rows, k * blk:(k + 1) * blk] = jnp.broadcast_to(
                tags[pl.ds(o * cap + k, 1), 0:blk], (tag_rows, blk)).astype(bf16)
        return carry

    lax.fori_loop(0, n_t, pack, 0)

    pl.semaphore_wait(barrier, n)

    def hidden_copy():
        start = pl.multiple_of(other * half, blk)
        return pltpu.make_async_remote_copy(
            src_ref=hidden.at[:, pl.ds(start, half)], dst_ref=peer_hidden,
            send_sem=ph_sem.at[0], recv_sem=ph_sem.at[1],
            device_id={"dp": other}, device_id_type=MESH)

    def packed_copy(o, src):
        return pltpu.make_async_remote_copy(
            src_ref=packed.at[o], dst_ref=landed.at[src],
            send_sem=pk_send.at[o], recv_sem=pk_recv.at[src],
            device_id={"tvoc": o}, device_id_type=MESH)

    def pack_send(q, carry):
        o = lax.rem(i + q, n_t)
        packed_copy(o, i).start()
        return carry

    lax.fori_loop(1, n_t, pack_send, 0)
    loads[1].wait()
    hidden_copy().start()

    loads[2].wait()
    depth = 4 * blk
    logits[...] = jnp.zeros_like(logits)

    def logit_step(k, carry):
        at = pl.multiple_of(k * depth, depth)
        logits[...] += jnp.dot(hidden[:, pl.ds(at, depth)], weight[pl.ds(at, depth), :], preferred_element_type=f32)
        return carry

    lax.fori_loop(0, width // depth, logit_step, 0)

    lg = logits[...]
    top = jnp.max(lg, axis=1, keepdims=True)
    e = jnp.exp(lg - top)
    e_sum = jnp.sum(e, axis=1, keepdims=True)
    shifted[...] = e


    own_at = d * half

    def turn_own(k, carry):
        at = pl.multiple_of(k * blk, blk)
        tile = hidden[:, pl.ds(pl.multiple_of(own_at + at, blk), blk)].astype(f32)
        hid_t[pl.ds(at, blk), 0:tokens] = tile.T.astype(bf16)
        return carry

    lax.fori_loop(0, half // blk, turn_own, 0)

    def add_mass(ref, o, first):
        for b in range(per_owner):
            acc = jnp.zeros((tokens, blk), f32) if first else mass[:, b * blk:(b + 1) * blk]
            for k in range(cap):
                which = ref[o, tokens:tokens + 1, k * blk:(k + 1) * blk].astype(f32)
                part = ref[o, 0:tokens, k * blk:(k + 1) * blk].astype(f32)
                acc = acc + jnp.where(which == float(b), part, 0.0)
            mass[:, b * blk:(b + 1) * blk] = acc

    add_mass(packed, i, True)

    def take_mass(q, carry):
        o = lax.rem(i + q, n_t)
        packed_copy(o, o).wait_recv()
        add_mass(landed, o, False)
        return carry

    lax.fori_loop(1, n_t, take_mass, 0)

    lg = logits[...]
    tm = mass[...]
    positive = tm > 0
    parts = (
        top,
        e_sum,
        jnp.sum(tm, axis=1, keepdims=True),
        jnp.sum(jnp.where(positive, tm * jnp.log(jnp.where(positive, tm, 1.0)), 0.0), axis=1, keepdims=True),
        jnp.sum(tm * lg, axis=1, keepdims=True),
    )
    spot = lax.broadcasted_iota(jnp.int32, (tokens, 128), 1)
    wide = jnp.zeros((tokens, 128), f32)
    for k, part in enumerate(parts):
        wide = jnp.where(spot == k, part, wide)
    stats[me] = wide.T[0:8]

    def stat_copy(q, src):
        r, where = peer(q)
        return pltpu.make_async_remote_copy(
            src_ref=stats.at[me], dst_ref=stats.at[src],
            send_sem=st_send.at[q], recv_sem=st_recv.at[src],
            device_id=where, device_id_type=MESH)

    def stat_send(q, carry):
        stat_copy(q, me).start()
        return carry

    lax.fori_loop(1, n, stat_send, 0)

    hidden_copy().wait_recv()

    def turn_peer(k, carry):
        at = pl.multiple_of(k * blk, blk)
        hid_t[pl.ds(at, blk), tokens:2 * tokens] = peer_hidden[:, pl.ds(at, blk)].astype(f32).T.astype(bf16)
        return carry

    lax.fori_loop(0, half // blk, turn_peer, 0)

    def stat_wait(q, carry):
        stat_copy(q, peer(q)[0]).wait_recv()
        return carry

    lax.fori_loop(1, n, stat_wait, 0)
    st = stats[...]
    largest = jnp.max(st, axis=0)[0:1]
    scale = jnp.exp(st[:, 0:1, :] - largest[None])
    line = lax.broadcasted_iota(jnp.int32, st.shape, 1)
    sums = jnp.sum(jnp.where(line == 1, st * scale, st), axis=0)
    total, mass_sum, entropy, cross = sums[1:2], sums[2:3], sums[3:4], sums[4:5]
    div_ref[...] = entropy / mass_sum - jnp.log(mass_sum) - cross / mass_sum + largest + jnp.log(total)
    rows8 = lax.broadcasted_iota(jnp.int32, (128, tokens), 0)
    back = jnp.where(rows8 == 0, largest, jnp.where(rows8 == 1, loss_scale / total, loss_scale / mass_sum)).T
    factor = jnp.exp(top - back[:, 0:1]) * back[:, 1:2]
    g = shifted[...] * factor - mass[...] * back[:, 2:3]
    grads[0:tokens, :] = g.astype(bf16)
    lg_copy = pltpu.make_async_remote_copy(
        src_ref=grads.at[pl.ds(0, tokens)], dst_ref=grads.at[pl.ds(tokens, tokens)],
        send_sem=lg_sem.at[0], recv_sem=lg_sem.at[1],
        device_id={"dp": other}, device_id_type=MESH)
    lg_copy.start()
    grad_t[...] = g.T.astype(bf16)

    direct = rows % 16 == 0
    if not direct:
        tile = 2 * blk

        def gh_step(k, carry):
            at = pl.multiple_of(k * tile, tile)
            gh_t[pl.ds(at, tile), :] = jnp.dot(weight[pl.ds(at, tile), :], grad_t[...], preferred_element_type=f32)
            return carry

        lax.fori_loop(0, width // tile, gh_step, 0)

    def chunk(ii, jj):
        start = (ii * n_s + jj) * rows
        if not direct:
            return gh_t[pl.ds(pl.multiple_of(start, 8), rows), :]
        return jnp.dot(weight[pl.ds(pl.multiple_of(start, 16), rows), :], grad_t[...], preferred_element_type=f32)

    def copy1(ii, jj, src):
        return pltpu.make_async_remote_copy(
            src_ref=out1.at[ii, jj], dst_ref=in1.at[src, jj],
            send_sem=s1.at[ii, jj], recv_sem=r1.at[src, jj],
            device_id={"tvoc": ii}, device_id_type=MESH)

    def copy2(jj, src):
        return pltpu.make_async_remote_copy(
            src_ref=out2.at[jj], dst_ref=in2.at[src],
            send_sem=s2.at[jj], recv_sem=r2.at[src],
            device_id={"svoc": jj}, device_id_type=MESH)

    def send1(p, carry):
        jj = lax.rem(j + p, n_s)

        def inner(q, c):
            ii = lax.rem(i + q, n_t)
            out1[ii, jj] = chunk(ii, jj).astype(bf16)
            copy1(ii, jj, i).start()
            return c

        return lax.fori_loop(1, n_t, inner, carry)

    lax.fori_loop(1, n_s + 1, send1, 0)

    def own_chunk(p, carry):
        jj = lax.rem(j + p, n_s)
        own_t[jj] = chunk(i, jj)
        return carry

    lax.fori_loop(1, n_s + 1, own_chunk, 0)

    lg_copy.wait_recv()

    tall = 2 * blk

    def gw_step(k, carry):
        at = pl.multiple_of(k * tall, tall)
        gw_ref[pl.ds(at, tall), :] = jnp.dot(
            hid_t[pl.ds(at, tall), :], grads[...], preferred_element_type=f32).astype(bf16)
        return carry

    lax.fori_loop(0, half // tall, gw_step, 0)

    def gather1(jj):
        acc = own_t[jj]
        for q in range(1, n_t):
            ii = lax.rem(i + q, n_t)
            copy1(ii, jj, ii).wait_recv()
            acc = acc + in1[ii, jj].astype(f32)
        return acc

    def send2(p, carry):
        jj = lax.rem(j + p, n_s)
        out2[jj] = gather1(jj).astype(bf16)
        copy2(jj, j).start()
        return carry

    lax.fori_loop(1, n_s, send2, 0)
    acc = gather1(j)
    for p in range(1, n_s):
        jj = lax.rem(j + p, n_s)
        copy2(jj, jj).wait_recv()
        acc = acc + in2[jj].astype(f32)
    gh_ref[...] = acc

    hidden_copy().wait_send()
    lg_copy.wait_send()

    def drain_packed(q, carry):
        o = lax.rem(i + q, n_t)
        packed_copy(o, i).wait_send()
        return carry

    lax.fori_loop(1, n_t, drain_packed, 0)

    def drain_stats(q, carry):
        stat_copy(q, me).wait_send()
        return carry

    lax.fori_loop(1, n, drain_stats, 0)

    def drain1(p, carry):
        jj = lax.rem(j + p, n_s)

        def inner(q, c):
            copy1(lax.rem(i + q, n_t), jj, i).wait_send()
            return c

        return lax.fori_loop(1, n_t, inner, carry)

    lax.fori_loop(1, n_s + 1, drain1, 0)

    def drain2(p, carry):
        copy2(lax.rem(j + p, n_s), j).wait_send()
        return carry

    lax.fori_loop(1, n_s, drain2, 0)


def local(n_t, n_s, teacher_probs, block_values, block_index, block_count, hidden, student_weight):
    tokens, width = hidden.shape
    slots, blk = block_values.shape[2], block_values.shape[3]
    shard = student_weight.shape[1]
    half, rows, n = width // 2, width // (n_t * n_s), n_t * n_s
    lanes = -(-(n_t * (shard // blk)) // 128) * 128
    vmem, smem = pl.BlockSpec(memory_space=pltpu.VMEM), pl.BlockSpec(memory_space=pltpu.SMEM)
    hbm = pl.BlockSpec(memory_space=pltpu.HBM)
    DMA = pltpu.SemaphoreType.DMA
    parcel = (n_t, tokens + tag_rows, cap * blk)
    div, gw, gh = pl.pallas_call(
        functools.partial(kernel, n_t, n_s, blk),
        out_shape=(
            jax.ShapeDtypeStruct((1, tokens), f32),
            jax.ShapeDtypeStruct((half, shard), bf16),
            jax.ShapeDtypeStruct((rows, tokens), f32),
        ),
        in_specs=[smem, smem, hbm, hbm, hbm, hbm],
        out_specs=(vmem, vmem, vmem),
        scratch_shapes=[
            pltpu.VMEM((teacher_probs.shape[1] // blk, tokens, blk), bf16),
            pltpu.VMEM(block_values.shape[2:], bf16),
            pltpu.VMEM(hidden.shape, bf16),
            pltpu.VMEM(student_weight.shape, bf16),
            pltpu.VMEM((tokens, half), bf16),
            pltpu.VMEM((half, 2 * tokens), bf16),
            pltpu.VMEM((slots, tokens, blk), f32),
            pltpu.VMEM((slots, lanes), f32),
            pltpu.VMEM((n_t * cap, lanes), f32),
            pltpu.VMEM(parcel, bf16),
            pltpu.VMEM(parcel, bf16),
            pltpu.VMEM((tokens, shard), f32),
            pltpu.VMEM((tokens, shard), f32),
            pltpu.VMEM((tokens, shard), f32),
            pltpu.VMEM((n, 8, tokens), f32),
            pltpu.VMEM((2 * tokens, shard), bf16),
            pltpu.VMEM((shard, tokens), bf16),
            pltpu.VMEM((width, tokens), f32),
            pltpu.VMEM((n_s, rows, tokens), f32),
            pltpu.VMEM((n_t, n_s, rows, tokens), bf16),
            pltpu.VMEM((n_t, n_s, rows, tokens), bf16),
            pltpu.VMEM((n_s, rows, tokens), bf16),
            pltpu.VMEM((n_s, rows, tokens), bf16),
            DMA((teacher_probs.shape[1] // blk,)), DMA((3,)), DMA((2,)), DMA((n_t,)), DMA((n_t,)), DMA((n,)), DMA((n,)), DMA((2,)),
            DMA((n_t, n_s)), DMA((n_t, n_s)), DMA((n_s,)), DMA((n_s,)),
        ],
        compiler_params=pltpu.CompilerParams(
            collective_id=0, has_side_effects=True, vmem_limit_bytes=67043328 - 7 * 2**18),
    )(jnp.swapaxes(block_index, 2, 3), block_count, teacher_probs, block_values, hidden, student_weight)
    return div.reshape(tokens), gw, gh.T


def solution(mesh):
    return jax.shard_map(
        functools.partial(local, mesh.shape["tvoc"], mesh.shape["svoc"]),
        mesh=mesh,
        in_specs=(
            P("dp", "tvoc"),
            P("tvoc", "svoc", None, None, None),
            P("tvoc", "svoc", None, None),
            P("tvoc", "svoc"),
            P("dp", None),
            P(None, ("tvoc", "svoc")),
        ),
        out_specs=(P("dp"), P("dp", ("tvoc", "svoc")), P("dp", ("tvoc", "svoc"))),
        check_vma=False,
    )
```

```python
import functools

import jax
import jax.numpy as jnp
from jax import lax
from jax.experimental import pallas as pl
from jax.experimental.pallas import tpu as pltpu
from jax.sharding import PartitionSpec as P

loss_scale = 128.0
cap = 2
tag_rows = 16
MESH = pl.DeviceIdType.MESH
f32, bf16 = jnp.float32, jnp.bfloat16


def kernel(
    n_t, n_s, blk,
    idx_s, cnt_s, teacher_hbm, values_hbm, hidden_hbm, weight_hbm,
    div_ref, gw_ref, gh_ref,
    teacher, values, hidden, weight, peer_hidden, hid_t, mapped, targets, tags,
    packed, landed, mass, logits, shifted, stats, grads, grad_t, gh_t, own_t, out1, in1, out2, in2,
    block_sem, load_sem, ph_sem, pk_send, pk_recv, st_send, st_recv, lg_sem, s1, r1, s2, r2,
):
    d, i, j = lax.axis_index("dp"), lax.axis_index("tvoc"), lax.axis_index("svoc")
    n_d = 2
    n = n_t * n_s
    me = i * n_s + j
    other = n_d - 1 - d
    tokens, width = hidden.shape
    shard = weight.shape[1]
    per_owner = shard // blk
    half = width // n_d
    rows = width // n

    slots, blocks = values.shape[0], teacher.shape[0]
    loads = [
        pltpu.make_async_copy(src, dst, load_sem.at[k])
        for k, (src, dst) in enumerate(((values_hbm.at[0, 0], values), (hidden_hbm, hidden), (weight_hbm, weight)))
    ]
    loads[0].start()

    def block_load(b):
        return pltpu.make_async_copy(
            teacher_hbm.at[:, pl.ds(pl.multiple_of(b * blk, blk), blk)], teacher.at[b], block_sem.at[b])

    def block_start(b, carry):
        block_load(b).start()
        return carry

    lax.fori_loop(0, blocks, block_start, 0)
    loads[1].start()
    loads[2].start()

    def peer(q):
        r = lax.rem(me + q, n)
        return r, {"tvoc": r // n_s, "svoc": lax.rem(r, n_s)}

    barrier = pltpu.get_barrier_semaphore()

    def greet(q, carry):
        pl.semaphore_signal(barrier, inc=1, device_id=peer(q)[1], device_id_type=MESH)
        return carry

    lax.fori_loop(1, n, greet, 0)
    pl.semaphore_signal(barrier, inc=1, device_id={"dp": other}, device_id_type=MESH)

    lanes = targets.shape[1]
    lane = lax.broadcasted_iota(jnp.int32, (slots, lanes), 1)
    slot = lax.broadcasted_iota(jnp.int32, (slots, lanes), 0)
    column = jnp.zeros((slots, lanes), jnp.int32)
    for s in range(slots):
        column = jnp.where(slot == s, idx_s[0, 0, 1, s], column)
    hot = (column == lane) & (slot < cnt_s[0, 0])
    present = jnp.max(jnp.where(hot, 1.0, 0.0), axis=0, keepdims=True)
    r_iota = lax.broadcasted_iota(jnp.int32, (lanes, lanes), 0).astype(f32)
    c_iota = lax.broadcasted_iota(jnp.int32, (lanes, lanes), 1).astype(f32)
    r_own = jnp.floor((r_iota + 0.5) / per_owner)
    c_own = jnp.floor((c_iota + 0.5) / per_owner)
    below = jnp.where((r_own == c_own) & (r_iota < c_iota), 1.0, 0.0)
    rank = jnp.dot(jnp.broadcast_to(present, (8, lanes)), below, preferred_element_type=f32)[0:1]
    place = cap * c_own[0:1] + rank
    goal = jnp.sum(jnp.where(hot, place + 1.0, 0.0), axis=1, keepdims=True) - 1.0
    targets[...] = jnp.broadcast_to(goal, (slots, lanes))
    n_tags = tags.shape[0]
    t_iota = lax.broadcasted_iota(jnp.int32, (n_tags, lanes), 0).astype(f32)
    within = c_iota[0:1] - per_owner * c_own[0:1]
    tag = jnp.sum(jnp.where((present > 0.0) & (place == t_iota), within + 1.0, 0.0), axis=1, keepdims=True) - 1.0
    tags[...] = jnp.broadcast_to(tag, (n_tags, lanes))

    def block_wait(b, carry):
        block_load(b).wait()
        return carry

    loads[0].wait()
    lax.fori_loop(0, blocks, block_wait, 0)
    for s in range(slots):
        mapped[s] = jnp.dot(teacher[idx_s[0, 0, 0, s]], values[s], preferred_element_type=f32)

    def pack(q, carry):
        o = lax.rem(i + q, n_t)
        for k in range(cap):
            t = (o * cap + k).astype(f32)
            acc = jnp.zeros((tokens, blk), f32)
            for s in range(slots):
                acc = acc + jnp.where(targets[s:s + 1, 0:blk] == t, mapped[s], 0.0)
            packed[o, 0:tokens, k * blk:(k + 1) * blk] = acc.astype(bf16)
            packed[o, tokens:tokens + tag_rows, k * blk:(k + 1) * blk] = jnp.broadcast_to(
                tags[pl.ds(o * cap + k, 1), 0:blk], (tag_rows, blk)).astype(bf16)
        return carry

    lax.fori_loop(1, n_t, pack, 0)

    pl.semaphore_wait(barrier, n)

    def hidden_copy():
        start = pl.multiple_of(other * half, blk)
        return pltpu.make_async_remote_copy(
            src_ref=hidden.at[:, pl.ds(start, half)], dst_ref=peer_hidden,
            send_sem=ph_sem.at[0], recv_sem=ph_sem.at[1],
            device_id={"dp": other}, device_id_type=MESH)

    def packed_copy(o, src):
        return pltpu.make_async_remote_copy(
            src_ref=packed.at[o], dst_ref=landed.at[src],
            send_sem=pk_send.at[o], recv_sem=pk_recv.at[src],
            device_id={"tvoc": o}, device_id_type=MESH)

    def pack_send(q, carry):
        o = lax.rem(i + q, n_t)
        packed_copy(o, i).start()
        return carry

    lax.fori_loop(1, n_t, pack_send, 0)
    loads[1].wait()
    hidden_copy().start()
    pack(0, 0)

    loads[2].wait()
    depth = 4 * blk
    logits[...] = jnp.zeros_like(logits)

    def logit_step(k, carry):
        at = pl.multiple_of(k * depth, depth)
        logits[...] += jnp.dot(hidden[:, pl.ds(at, depth)], weight[pl.ds(at, depth), :], preferred_element_type=f32)
        return carry

    lax.fori_loop(0, width // depth, logit_step, 0)

    lg = logits[...]
    top = jnp.max(lg, axis=1, keepdims=True)
    e = jnp.exp(lg - top)
    e_sum = jnp.sum(e, axis=1, keepdims=True)
    shifted[...] = e


    own_at = d * half

    def turn_own(k, carry):
        at = pl.multiple_of(k * blk, blk)
        tile = hidden[:, pl.ds(pl.multiple_of(own_at + at, blk), blk)].astype(f32)
        hid_t[pl.ds(at, blk), 0:tokens] = tile.T.astype(bf16)
        return carry

    lax.fori_loop(0, half // blk, turn_own, 0)

    def add_mass(ref, o, first):
        for b in range(per_owner):
            acc = jnp.zeros((tokens, blk), f32) if first else mass[:, b * blk:(b + 1) * blk]
            for k in range(cap):
                which = ref[o, tokens:tokens + 1, k * blk:(k + 1) * blk].astype(f32)
                part = ref[o, 0:tokens, k * blk:(k + 1) * blk].astype(f32)
                acc = acc + jnp.where(which == float(b), part, 0.0)
            mass[:, b * blk:(b + 1) * blk] = acc

    add_mass(packed, i, True)

    def take_mass(q, carry):
        o = lax.rem(i + q, n_t)
        packed_copy(o, o).wait_recv()
        add_mass(landed, o, False)
        return carry

    lax.fori_loop(1, n_t, take_mass, 0)

    lg = logits[...]
    tm = mass[...]
    positive = tm > 0
    parts = (
        top,
        e_sum,
        jnp.sum(tm, axis=1, keepdims=True),
        jnp.sum(jnp.where(positive, tm * jnp.log(jnp.where(positive, tm, 1.0)), 0.0), axis=1, keepdims=True),
        jnp.sum(tm * lg, axis=1, keepdims=True),
    )
    spot = lax.broadcasted_iota(jnp.int32, (tokens, 128), 1)
    wide = jnp.zeros((tokens, 128), f32)
    for k, part in enumerate(parts):
        wide = jnp.where(spot == k, part, wide)
    stats[me] = wide.T[0:8]

    def stat_copy(q, src):
        r, where = peer(q)
        return pltpu.make_async_remote_copy(
            src_ref=stats.at[me], dst_ref=stats.at[src],
            send_sem=st_send.at[q], recv_sem=st_recv.at[src],
            device_id=where, device_id_type=MESH)

    def stat_send(q, carry):
        stat_copy(q, me).start()
        return carry

    lax.fori_loop(1, n, stat_send, 0)

    hidden_copy().wait_recv()

    def turn_peer(k, carry):
        at = pl.multiple_of(k * blk, blk)
        hid_t[pl.ds(at, blk), tokens:2 * tokens] = peer_hidden[:, pl.ds(at, blk)].astype(f32).T.astype(bf16)
        return carry

    lax.fori_loop(0, half // blk, turn_peer, 0)

    def stat_wait(q, carry):
        stat_copy(q, peer(q)[0]).wait_recv()
        return carry

    lax.fori_loop(1, n, stat_wait, 0)
    st = stats[...]
    largest = jnp.max(st, axis=0)[0:1]
    scale = jnp.exp(st[:, 0:1, :] - largest[None])
    line = lax.broadcasted_iota(jnp.int32, st.shape, 1)
    sums = jnp.sum(jnp.where(line == 1, st * scale, st), axis=0)
    total, mass_sum, entropy, cross = sums[1:2], sums[2:3], sums[3:4], sums[4:5]
    div_ref[...] = entropy / mass_sum - jnp.log(mass_sum) - cross / mass_sum + largest + jnp.log(total)
    rows8 = lax.broadcasted_iota(jnp.int32, (128, tokens), 0)
    back = jnp.where(rows8 == 0, largest, jnp.where(rows8 == 1, loss_scale / total, loss_scale / mass_sum)).T
    factor = jnp.exp(top - back[:, 0:1]) * back[:, 1:2]
    g = shifted[...] * factor - mass[...] * back[:, 2:3]
    grads[0:tokens, :] = g.astype(bf16)
    lg_copy = pltpu.make_async_remote_copy(
        src_ref=grads.at[pl.ds(0, tokens)], dst_ref=grads.at[pl.ds(tokens, tokens)],
        send_sem=lg_sem.at[0], recv_sem=lg_sem.at[1],
        device_id={"dp": other}, device_id_type=MESH)
    lg_copy.start()
    grad_t[...] = g.T.astype(bf16)

    direct = rows % 16 == 0
    if not direct:
        tile = 2 * blk

        def gh_step(k, carry):
            at = pl.multiple_of(k * tile, tile)
            gh_t[pl.ds(at, tile), :] = jnp.dot(weight[pl.ds(at, tile), :], grad_t[...], preferred_element_type=f32)
            return carry

        lax.fori_loop(0, width // tile, gh_step, 0)

    def chunk(ii, jj):
        start = (ii * n_s + jj) * rows
        if not direct:
            return gh_t[pl.ds(pl.multiple_of(start, 8), rows), :]
        return jnp.dot(weight[pl.ds(pl.multiple_of(start, 16), rows), :], grad_t[...], preferred_element_type=f32)

    def copy1(ii, jj, src):
        return pltpu.make_async_remote_copy(
            src_ref=out1.at[ii, jj], dst_ref=in1.at[src, jj],
            send_sem=s1.at[ii, jj], recv_sem=r1.at[src, jj],
            device_id={"tvoc": ii}, device_id_type=MESH)

    def copy2(jj, src):
        return pltpu.make_async_remote_copy(
            src_ref=out2.at[jj], dst_ref=in2.at[src],
            send_sem=s2.at[jj], recv_sem=r2.at[src],
            device_id={"svoc": jj}, device_id_type=MESH)

    def send1(p, carry):
        jj = lax.rem(j + p, n_s)

        def inner(q, c):
            ii = lax.rem(i + q, n_t)
            out1[ii, jj] = chunk(ii, jj).astype(bf16)
            copy1(ii, jj, i).start()
            return c

        return lax.fori_loop(1, n_t, inner, carry)

    lax.fori_loop(1, n_s + 1, send1, 0)

    def own_chunk(p, carry):
        jj = lax.rem(j + p, n_s)
        own_t[jj] = chunk(i, jj)
        return carry

    lax.fori_loop(1, n_s + 1, own_chunk, 0)

    lg_copy.wait_recv()

    tall = 2 * blk

    def gw_step(k, carry):
        at = pl.multiple_of(k * tall, tall)
        gw_ref[pl.ds(at, tall), :] = jnp.dot(
            hid_t[pl.ds(at, tall), :], grads[...], preferred_element_type=f32).astype(bf16)
        return carry

    lax.fori_loop(0, half // tall, gw_step, 0)

    def gather1(jj):
        acc = own_t[jj]
        for q in range(1, n_t):
            ii = lax.rem(i + q, n_t)
            copy1(ii, jj, ii).wait_recv()
            acc = acc + in1[ii, jj].astype(f32)
        return acc

    def send2(p, carry):
        jj = lax.rem(j + p, n_s)
        out2[jj] = gather1(jj).astype(bf16)
        copy2(jj, j).start()
        return carry

    lax.fori_loop(1, n_s, send2, 0)
    acc = gather1(j)
    for p in range(1, n_s):
        jj = lax.rem(j + p, n_s)
        copy2(jj, jj).wait_recv()
        acc = acc + in2[jj].astype(f32)
    gh_ref[...] = acc

    hidden_copy().wait_send()
    lg_copy.wait_send()

    def drain_packed(q, carry):
        o = lax.rem(i + q, n_t)
        packed_copy(o, i).wait_send()
        return carry

    lax.fori_loop(1, n_t, drain_packed, 0)

    def drain_stats(q, carry):
        stat_copy(q, me).wait_send()
        return carry

    lax.fori_loop(1, n, drain_stats, 0)

    def drain1(p, carry):
        jj = lax.rem(j + p, n_s)

        def inner(q, c):
            copy1(lax.rem(i + q, n_t), jj, i).wait_send()
            return c

        return lax.fori_loop(1, n_t, inner, carry)

    lax.fori_loop(1, n_s + 1, drain1, 0)

    def drain2(p, carry):
        copy2(lax.rem(j + p, n_s), j).wait_send()
        return carry

    lax.fori_loop(1, n_s, drain2, 0)


def flush(div, gw, gh, div_out, gw_out, gh_out, sem):
    copies = [
        pltpu.make_async_copy(src, dst, sem.at[k])
        for k, (src, dst) in enumerate(((gw, gw_out), (gh, gh_out), (div, div_out)))
    ]
    for copy in copies:
        copy.start()
    for copy in copies:
        copy.wait()


def local(n_t, n_s, teacher_probs, block_values, block_index, block_count, hidden, student_weight):
    tokens, width = hidden.shape
    slots, blk = block_values.shape[2], block_values.shape[3]
    shard = student_weight.shape[1]
    half, rows, n = width // 2, width // (n_t * n_s), n_t * n_s
    lanes = -(-(n_t * (shard // blk)) // 128) * 128
    vmem, smem = pl.BlockSpec(memory_space=pltpu.VMEM), pl.BlockSpec(memory_space=pltpu.SMEM)
    hbm = pl.BlockSpec(memory_space=pltpu.HBM)
    DMA = pltpu.SemaphoreType.DMA
    parcel = (n_t, tokens + tag_rows, cap * blk)
    div, gw, gh = pl.pallas_call(
        functools.partial(kernel, n_t, n_s, blk),
        out_shape=(
            jax.ShapeDtypeStruct((1, tokens), f32),
            jax.ShapeDtypeStruct((half, shard), bf16),
            jax.ShapeDtypeStruct((rows, tokens), f32),
        ),
        in_specs=[smem, smem, hbm, hbm, hbm, hbm],
        out_specs=(vmem, vmem, vmem),
        scratch_shapes=[
            pltpu.VMEM((teacher_probs.shape[1] // blk, tokens, blk), bf16),
            pltpu.VMEM(block_values.shape[2:], bf16),
            pltpu.VMEM(hidden.shape, bf16),
            pltpu.VMEM(student_weight.shape, bf16),
            pltpu.VMEM((tokens, half), bf16),
            pltpu.VMEM((half, 2 * tokens), bf16),
            pltpu.VMEM((slots, tokens, blk), f32),
            pltpu.VMEM((slots, lanes), f32),
            pltpu.VMEM((n_t * cap, lanes), f32),
            pltpu.VMEM(parcel, bf16),
            pltpu.VMEM(parcel, bf16),
            pltpu.VMEM((tokens, shard), f32),
            pltpu.VMEM((tokens, shard), f32),
            pltpu.VMEM((tokens, shard), f32),
            pltpu.VMEM((n, 8, tokens), f32),
            pltpu.VMEM((2 * tokens, shard), bf16),
            pltpu.VMEM((shard, tokens), bf16),
            pltpu.VMEM((width, tokens), f32),
            pltpu.VMEM((n_s, rows, tokens), f32),
            pltpu.VMEM((n_t, n_s, rows, tokens), bf16),
            pltpu.VMEM((n_t, n_s, rows, tokens), bf16),
            pltpu.VMEM((n_s, rows, tokens), bf16),
            pltpu.VMEM((n_s, rows, tokens), bf16),
            DMA((teacher_probs.shape[1] // blk,)), DMA((3,)), DMA((2,)), DMA((n_t,)), DMA((n_t,)), DMA((n,)), DMA((n,)), DMA((2,)),
            DMA((n_t, n_s)), DMA((n_t, n_s)), DMA((n_s,)), DMA((n_s,)),
        ],
        compiler_params=pltpu.CompilerParams(
            collective_id=0, has_side_effects=True, vmem_limit_bytes=32 * 1024 * 1024),
    )(
        pltpu.with_memory_space_constraint(jnp.swapaxes(block_index, 2, 3), pltpu.HBM), block_count,
        *(pltpu.with_memory_space_constraint(x, pltpu.HBM) for x in (teacher_probs, block_values, hidden, student_weight)))
    div, gw, gh = pl.pallas_call(
        flush,
        out_shape=tuple(jax.ShapeDtypeStruct(x.shape, x.dtype) for x in (div, gw, gh)),
        in_specs=[vmem] * 3,
        out_specs=(hbm,) * 3,
        scratch_shapes=[DMA((3,))],
        compiler_params=pltpu.CompilerParams(vmem_limit_bytes=2**20),
    )(div, gw, gh)
    return div.reshape(tokens), gw, gh.T


def solution(mesh):
    return jax.shard_map(
        functools.partial(local, mesh.shape["tvoc"], mesh.shape["svoc"]),
        mesh=mesh,
        in_specs=(
            P("dp", "tvoc"),
            P("tvoc", "svoc", None, None, None),
            P("tvoc", "svoc", None, None),
            P("tvoc", "svoc"),
            P("dp", None),
            P(None, ("tvoc", "svoc")),
        ),
        out_specs=(P("dp"), P("dp", ("tvoc", "svoc")), P("dp", ("tvoc", "svoc"))),
        check_vma=False,
    )
```
